8 devices in a mesh: dp: 2 (over y, z), ep: 4 (over x, core).
Axes of the slice: x: 2, y: 2, z: 1, core: 2. Of those that a mesh axis runs over, the one named last changes fastest.
Arguments:
- x: bfloat16 [2, 4, 512, 2048], P('dp', 'ep'), parts along dimension 0
- expert: int32 [2, 4, 512, 8], P('dp', 'ep'), parts along dimension 0
- slot: int32 [2, 4, 512, 8], P('dp', 'ep'), parts along dimension 0
- gate: float32 [2, 4, 512, 8], P('dp', 'ep'), parts along dimension 0
- w_gate: bfloat16 [64, 2048, 1024], P('ep')
- w_up: bfloat16 [64, 2048, 1024], P('ep')
- w_down: bfloat16 [64, 1024, 2048], P('ep')
Outputs:
- y: bfloat16 [2, 4, 512, 2048], P('dp', 'ep'), parts along dimension 0
There are 2 independent parts. The reference program is written for one: setup_inputs(seed, part) draws one part's arguments, and reference() takes and returns one part's arrays. A program takes and returns all parts, laid end to end along the dimension named above; an argument that names none is the same for every part.
All inputs are finite; a program needn't handle non-finite values.
Results may differ from the reference program's by a relative error of at most 0.009.
Values are sent between devices in bfloat16 or wider.
A program may use at most 2 GiB of HBM per device.

```python
import jax
import jax.numpy as jnp

MEMBERS = 4
TOKENS = 512
D = 2048
FF = 1024
TOP = 8
EXPERTS = 64
SLOTS = 5 * TOKENS * TOP // (4 * EXPERTS)


def setup_inputs(seed: int = 0, part: int = 0) -> dict:
    own, k1, k2, k3, k4, k5, k6 = jax.random.split(jax.random.key(seed), 7)
    kx, ke, kl, kg = jax.random.split(jax.random.fold_in(own, part), 4)
    devices = (1, MEMBERS)
    place = jax.random.permutation(kl, jnp.arange(EXPERTS, dtype=jnp.uint32))
    slow = ((EXPERTS + (9 * place) % EXPERTS) << ((9 * place) // EXPERTS)) // EXPERTS
    wait = (jax.random.bits(ke, (*devices, TOKENS, EXPERTS), jnp.uint32) >> 10) * slow
    expert = jnp.argsort(wait, axis=-1)[..., :TOP].astype(jnp.int32)
    chosen = jax.nn.one_hot(expert, EXPERTS, dtype=jnp.int32)
    in_line = jnp.cumsum(chosen.reshape(*devices, TOKENS * TOP, EXPERTS), axis=2) - 1
    slot = jnp.sum(in_line.reshape(chosen.shape) * chosen, axis=-1)

    def one(key, rows, columns):
        return (jax.random.normal(key, (rows, columns), jnp.float32) * rows**-0.5).astype(jnp.bfloat16)

    def weights(key, rows, columns):
        return jax.lax.map(lambda k: one(k, rows, columns), jax.random.split(key, EXPERTS))

    return {
        "x": jax.random.normal(kx, (*devices, TOKENS, D), jnp.float32).astype(jnp.bfloat16),
        "expert": expert,
        "slot": slot,
        "gate": jax.nn.softmax(jax.random.normal(kg, expert.shape, jnp.float32)),
        "w_gate": weights(k1, D, FF),
        "w_up": weights(k2, D, FF),
        "w_down": weights(k3, FF, D),
    }


def einsum(form, a, b):
    return jnp.einsum(form, a.astype(jnp.float32), b.astype(jnp.float32))


def reference(x, expert, slot, gate, w_gate, w_up, w_down):
    to_expert = jax.nn.one_hot(expert, EXPERTS, dtype=jnp.bfloat16)
    to_slot = jax.nn.one_hot(slot, SLOTS, dtype=jnp.bfloat16)
    weighted = to_expert * gate[..., None].astype(jnp.bfloat16)
    dispatch = einsum("abtke,abtkc->abtec", to_expert, to_slot).astype(jnp.bfloat16)
    combine = einsum("abtke,abtkc->abtec", weighted, to_slot).astype(jnp.bfloat16)
    z = einsum("abtec,abtd->aebcd", dispatch, x).astype(jnp.bfloat16)
    h = jax.nn.silu(einsum("aebcd,edf->aebcf", z, w_gate))
    h = (h * einsum("aebcd,edf->aebcf", z, w_up)).astype(jnp.bfloat16)
    out = einsum("aebcf,efd->aebcd", h, w_down).astype(jnp.bfloat16)
    y = einsum("abtec,aebcd->abtd", combine, out)
    return y.astype(jnp.bfloat16)
```

```python
import functools

import jax
import jax.numpy as jnp
from jax import lax
from jax.experimental import pallas as pl
from jax.experimental.pallas import tpu as pltpu
from jax.sharding import PartitionSpec as P


F32, BF16 = jnp.float32, jnp.bfloat16


def slots_of(expert, slot, e):
    return jnp.max(jnp.where(expert == e, slot, -1), axis=0, keepdims=True)


def gates_of(expert, gate, e):
    return jnp.sum(jnp.where(expert == e, gate, 0.0), axis=0, keepdims=True)


def up_kernel(parts, cap, fblk, e_ref, s_ref, *refs):
    n = sum(len(p) for p in parts)
    xs, (wg_ref, wu_ref, h_ref, z_ref) = refs[:n], refs[n:]
    e = pl.program_id(0)
    rows = lax.broadcasted_iota(jnp.int32, (cap, e_ref.shape[2]), 0)
    k = 0
    for i, part in enumerate(parts):
        sl = slots_of(e_ref[i], s_ref[i], e)
        pick = jnp.where(rows == sl, 1.0, 0.0).astype(BF16)
        z, at = None, 0
        for tokens in part:
            d = jnp.dot(pick[:, at : at + tokens], xs[k][...], preferred_element_type=F32)
            z, at, k = d if z is None else z + d, at + tokens, k + 1
        z_ref[pl.ds(i * cap, cap), :] = z.astype(BF16)
    for f in range(0, wg_ref.shape[2], fblk):
        g = jnp.dot(z_ref[...], wg_ref[0, :, f : f + fblk], preferred_element_type=F32)
        u = jnp.dot(z_ref[...], wu_ref[0, :, f : f + fblk], preferred_element_type=F32)
        h_ref[0, :, f : f + fblk] = (g * jax.nn.sigmoid(g) * u).astype(BF16)


def up(expert, slot, xs, parts, w_gate, w_up, cap, fblk=256):
    n_e, d, ff = w_gate.shape
    s, _, tokens = expert.shape
    whole = lambda a: pl.BlockSpec(a.shape, lambda e: (0,) * a.ndim, pipeline_mode=pl.Buffered(1))
    return pl.pallas_call(
        functools.partial(up_kernel, parts, cap, fblk),
        grid=(n_e,),
        out_shape=jax.ShapeDtypeStruct((n_e, s * cap, ff), BF16),
        in_specs=[whole(expert), whole(slot)]
        + [whole(x) for x in xs]
        + [pl.BlockSpec((1, d, ff), lambda e: (e, 0, 0))] * 2,
        out_specs=pl.BlockSpec((1, s * cap, ff), lambda e: (e, 0, 0)),
        scratch_shapes=[pltpu.VMEM((s * cap, d), BF16)],
        cost_estimate=pl.CostEstimate(
            flops=n_e * s * cap * d * (4 * ff + 2 * tokens),
            bytes_accessed=4 * n_e * d * ff,
            transcendentals=n_e * s * cap * ff,
        ),
    )(expert, slot, *xs, w_gate, w_up)


def down_kernel(cap, eb, e_ref, s_ref, g_ref, h_ref, w_ref, o0_ref, o1_ref, out_ref, c_ref):
    step = pl.program_id(0)
    outs = (o0_ref, o1_ref)
    rows = lax.broadcasted_iota(jnp.int32, (cap, e_ref.shape[2]), 0)
    for b in range(eb):
        e = step * eb + b
        at = pl.multiple_of(e * cap, cap)
        o = jnp.dot(h_ref[e], w_ref[b], preferred_element_type=F32).astype(BF16)
        for i in range(len(outs)):
            sl = slots_of(e_ref[i], s_ref[i], e)
            ga = gates_of(e_ref[i], g_ref[i], e)
            c_ref[i, pl.ds(at, cap), :] = jnp.where(rows == sl, ga, 0.0).astype(BF16)
            out_ref[i, pl.ds(at, cap), :] = o[i * cap : (i + 1) * cap]

    @pl.when(step == pl.num_programs(0) - 1)
    def _():
        for i, o_ref in enumerate(outs):
            for t in range(0, o_ref.shape[0], 256):
                y = lax.dot_general(
                    c_ref[i, :, t : t + 256], out_ref[i], (((0,), (0,)), ((), ())),
                    preferred_element_type=F32,
                )
                o_ref[t : t + 256, :] = y.astype(o_ref.dtype)


def down(expert, slot, gate, h, w_down, start, cols, cap, eb):
    n_e, ff, _ = w_down.shape
    s, _, tokens = expert.shape
    at = start // cols
    assert at * cols == start
    whole = lambda a: pl.BlockSpec(a.shape, lambda e: (0,) * a.ndim, pipeline_mode=pl.Buffered(1))
    out = pl.BlockSpec((tokens, cols), lambda e: (0, 0), pipeline_mode=pl.Buffered(1))
    return pl.pallas_call(
        functools.partial(down_kernel, cap, eb),
        grid=(n_e // eb,),
        out_shape=[
            jax.ShapeDtypeStruct((tokens, cols), F32),
            jax.ShapeDtypeStruct((tokens, cols), BF16),
        ],
        in_specs=[whole(expert), whole(slot), whole(gate), whole(h),
                  pl.BlockSpec((eb, ff, cols), lambda e: (e, 0, at))],
        out_specs=[out, out],
        scratch_shapes=[
            pltpu.VMEM((s, n_e * cap, cols), BF16),
            pltpu.VMEM((s, n_e * cap, tokens), BF16),
        ],
        cost_estimate=pl.CostEstimate(
            flops=2 * n_e * s * cap * cols * (ff + tokens),
            bytes_accessed=2 * n_e * cols * ff,
            transcendentals=0,
        ),
    )(expert, slot, gate, h, w_down)


def solution(mesh):
    members = mesh.shape["ep"]

    def local(x, expert, slot, gate, w_gate, w_up, w_down):
        x = x[0, 0]
        tokens, d = x.shape
        top = expert.shape[-1]
        n_e = w_gate.shape[0]
        cap = 5 * tokens * top // (4 * n_e * members)
        me = lax.axis_index("ep")

        def cross(v):
            return lax.ppermute(v, "ep", [(i, i ^ 2) for i in range(members)])

        def sibling(v):
            return lax.ppermute(v, "ep", [(i, i ^ 1) for i in range(members)])

        meta = jnp.concatenate(
            [expert[0, 0].T.astype(F32), jnp.minimum(slot[0, 0], cap).T.astype(F32),
             gate[0, 0].T.astype(BF16).astype(F32)], axis=0)
        cross_x = [cross(x[: tokens // 2]), cross(x[tokens // 2 :])]
        sib_x = sibling(x)
        metas = lax.all_gather(meta, "ep")

        def routing(sources):
            m = jnp.stack([lax.dynamic_index_in_dim(metas, i, keepdims=False) for i in sources])
            return (m[:, :top].astype(jnp.int32) - me * n_e, m[:, top : 2 * top].astype(jnp.int32),
                    m[:, 2 * top :])

        le, ls, lg = routing([me, me ^ 1])
        re, rs, rg = routing([me ^ 2, me ^ 3])

        h_l = up(le, ls, [x, sib_x], [[tokens], [tokens]], w_gate, w_up, cap)
        cross_x, h_l = lax.optimization_barrier((cross_x, h_l))
        fwd_x = [sibling(v) for v in cross_x]
        half = [v.shape[0] for v in cross_x]
        h_r = up(re, rs, cross_x + fwd_x, [half, half], w_gate, w_up, cap)

        both, back = [], []
        for n, (start, cols) in enumerate(((0, 256), (256, 256), (512, 512), (1024, 1024))):
            mine, other = down(re, rs, rg, h_r, w_down, start, cols, cap, 2048 // cols)
            if n:
                mine, other, both[-1] = lax.optimization_barrier((mine, other, both[-1]))
                back.append(cross(both[-1]))
            both.append((mine + sibling(other).astype(F32)).astype(BF16))
            h_r, _ = lax.optimization_barrier((h_r, mine))
        h_l, _ = lax.optimization_barrier((h_l, mine))
        own0, other0 = down(le, ls, lg, h_l, w_down, 0, d // 2, cap, 2)
        own0, other0, both[-1] = lax.optimization_barrier((own0, other0, both[-1]))
        back.append(cross(both[-1]))
        h_l, _ = lax.optimization_barrier((h_l, own0))
        own1, other1 = down(le, ls, lg, h_l, w_down, d // 2, d // 2, cap, 2)
        other = jnp.concatenate([sibling(other0), sibling(other1)], axis=1)
        y = jnp.concatenate([own0, own1], axis=1) + other.astype(F32) + jnp.concatenate(back, axis=1).astype(F32)
        return y.astype(BF16)[None, None]

    tok = P("dp", "ep", None, None)
    w = P("ep", None, None)

    return jax.shard_map(local, mesh=mesh, in_specs=(tok,) * 4 + (w,) * 3, out_specs=tok, check_vma=False)
```

```python
import functools

import jax
import jax.numpy as jnp
from jax import lax
from jax.experimental import pallas as pl
from jax.experimental.pallas import tpu as pltpu
from jax.sharding import PartitionSpec as P

F32, BF16 = jnp.float32, jnp.bfloat16
MESH = pl.DeviceIdType.MESH

EARLY = 6
RING, DRING = 8, 4
KC, CC, FB = 512, 512, 256


def moe_kernel(cap, meta_ref, x_ref, wg_ref, wu_ref, wd_ref, own_ref, sibr_ref, crossr_ref,
               metas, xs, wgr, wur, wdr, hl, hr, sibrecv, zr, zl,
               gsem, usem, dsem, xsem, msend, mrecv, xsend, xrecv,
               qsend_sem, qrecv_sem, csend_sem, crecv_sem, lsend_sem, lrecv_sem, osem):
    me = lax.axis_index("ep")
    sib = me + 1 - 2 * (me % 2)
    far = (me + 2) % 4
    peers = (sib, far, (sib + 2) % 4)
    n_e, d, ff = wg_ref.shape
    top, tokens = metas.shape[1] // 3, metas.shape[2]
    nk, nc = d // KC, d // CC
    first = me * n_e

    barrier = pltpu.get_barrier_semaphore()
    for p in peers:
        pl.semaphore_signal(barrier, inc=1, device_id={"ep": p}, device_id_type=MESH)

    late = n_e - EARLY
    phases = [("L", 0, 4 * EARLY)] + [("R", k, n_e) for k in range(nk)] + [("L", EARLY, 4 * late)]
    bases = [sum(p[2] for p in phases[:i]) for i in range(len(phases))]
    total = bases[-1] + phases[-1][2]

    def piece(pos, lo):
        def inside(i):
            kind, a, _ = phases[i]
            at = pos - bases[i]
            return (a + at // 4, at % 4) if kind == "L" else (at, a)
        e, k = inside(lo)
        if lo + 1 < len(phases):
            nxt = pos // bases[lo + 1]
            e1, k1 = inside(lo + 1)
            e, k = e + nxt * (e1 - e), k + nxt * (k1 - k)
        return e, k

    def fill(pos, e, k):
        slot = pos % RING
        rows = pl.ds(pl.multiple_of(k * KC, KC), KC)
        pltpu.make_async_copy(wg_ref.at[e, rows], wgr.at[slot], gsem.at[slot]).start()
        pltpu.make_async_copy(wu_ref.at[e, rows], wur.at[slot], usem.at[slot]).start()

    def filled(slot):
        pltpu.make_async_copy(wg_ref.at[0, pl.ds(0, KC)], wgr.at[slot], gsem.at[slot]).wait()
        pltpu.make_async_copy(wu_ref.at[0, pl.ds(0, KC)], wur.at[slot], usem.at[slot]).wait()

    def dfill(pos):
        slot, e, c = pos % DRING, pos % n_e, (pos // n_e) % nc
        cols = pl.ds(pl.multiple_of(c * CC, CC), CC)
        pltpu.make_async_copy(wd_ref.at[e, :, cols], wdr.at[slot], dsem.at[slot]).start()

    def dfilled(slot):
        pltpu.make_async_copy(wd_ref.at[0, :, pl.ds(0, CC)], wdr.at[slot], dsem.at[slot]).wait()

    def x_local(k):
        return pltpu.make_async_copy(x_ref.at[:, pl.ds(k * KC, KC)], xs.at[0, k], xsem.at[k])

    def x_copy(src, k):
        piece_ref = xs.at[2, k] if src == 3 else x_ref.at[:, pl.ds(k * KC, KC)]
        return pltpu.make_async_remote_copy(
            src_ref=piece_ref, dst_ref=xs.at[src, k], send_sem=xsend.at[src - 1, k],
            recv_sem=xrecv.at[src - 1, k], device_id={"ep": far if src == 2 else sib}, device_id_type=MESH)

    def meta_copy(src):
        return pltpu.make_async_remote_copy(
            src_ref=meta_ref, dst_ref=metas.at[src], send_sem=msend.at[src - 1],
            recv_sem=mrecv.at[src - 1], device_id={"ep": peers[src - 1]}, device_id_type=MESH)

    for k in range(nk):
        x_local(k).start()
    for pos in range(RING):
        fill(pos, pos // 4, pos % 4)
    metas[0] = meta_ref[...]
    pl.semaphore_wait(barrier, 3)
    for src in (1, 2, 3):
        meta_copy(src).start()
    for k in range(nk):
        x_copy(1, k).start()
    for k in range(nk):
        x_copy(2, k).start()

    slot_rows = lax.broadcasted_iota(jnp.int32, (cap, tokens), 0).astype(F32)

    def slots_of(src, e):
        hit = metas[src, 0:top, :] == (e + first).astype(F32)
        return jnp.max(jnp.where(hit, metas[src, top : 2 * top, :], -1.0), axis=0, keepdims=True)

    def gates_of(src, e):
        hit = metas[src, 0:top, :] == (e + first).astype(F32)
        return jnp.sum(jnp.where(hit, metas[src, 2 * top :, :], 0.0), axis=0, keepdims=True)

    def pick(src, e):
        return jnp.where(slot_rows == slots_of(src, e), 1.0, 0.0).astype(BF16)

    def dot(a, b):
        return jnp.dot(a, b, preferred_element_type=F32)

    def near(lo, count, after):
        _, e0, _ = phases[lo]

        def body(i, _):
            e = e0 + i
            for s in (0, 1):
                p = pick(s, e)
                for k in range(nk):
                    zl[s * cap : (s + 1) * cap, k * KC : (k + 1) * KC] = dot(p, xs[s, k]).astype(BF16)
            pos = bases[lo] + 4 * i
            at = pl.multiple_of(pos % RING, 4)
            for q in range(4):
                filled(at + q)
            for f in range(0, ff, FB):
                wg = wgr[pl.ds(at, 4), :, f : f + FB].reshape(d, FB)
                wu = wur[pl.ds(at, 4), :, f : f + FB].reshape(d, FB)
                g, u = dot(zl[...], wg), dot(zl[...], wu)
                hl[e, :, f : f + FB] = (g * jax.nn.sigmoid(g) * u).astype(BF16)

            def refill():
                for q in range(4):
                    nxt = pos + q + RING
                    fill(nxt, *piece(nxt, lo))

            if lo + 1 < len(phases):
                refill()
            else:
                pl.when(i < count - 2)(refill)
            after(i)
            return 0

        lax.fori_loop(0, count, body, 0)

    def pass_on(k):
        x_copy(2, k).wait_recv()
        x_copy(3, k).start()

    def far_phase(k, acc):
        lo = 1 + k
        x_copy(3, k).wait_recv()

        def body(i, _):
            if k + 1 < nk:
                @pl.when(i == n_e // 2 - 1)
                def _():
                    pass_on(k + 1)
            for b in (0, 1):
                for s in (0, 1):
                    zr[b, s * cap : (s + 1) * cap, :] = dot(pick(2 + s, 2 * i + b), xs[2 + s, k]).astype(BF16)
            for b in (0, 1):
                e = 2 * i + b
                pos = bases[lo] + e
                slot = pos % RING
                filled(slot)
                for f in range(0, ff, FB):
                    g = dot(zr[b], wgr[slot, :, f : f + FB])
                    u = dot(zr[b], wur[slot, :, f : f + FB])
                    if k:
                        g = g + acc[e, :, f : f + FB]
                        u = u + acc[e, :, ff + f : ff + f + FB]
                    if k == nk - 1:
                        hr[e, :, f : f + FB] = (g * jax.nn.sigmoid(g) * u).astype(BF16)
                    else:
                        acc[e, :, f : f + FB] = g
                        acc[e, :, ff + f : ff + f + FB] = u
                fill(pos + RING, *piece(pos + RING, lo))
            return 0

        lax.fori_loop(0, n_e // 2, body, 0)

    for k in range(nk):
        x_local(k).wait()
        x_copy(1, k).wait_recv()
    meta_copy(1).wait_recv()

    def first_pass_on(i):
        @pl.when(i == EARLY - 2)
        def _():
            pass_on(0)

    near(0, EARLY, first_pass_on)
    for pos in range(DRING):
        dfill(pos)
    meta_copy(2).wait_recv()
    meta_copy(3).wait_recv()

    def first_half(acc):
        for k in range(nk):
            far_phase(k, acc)

    pl.run_scoped(first_half, pltpu.VMEM((n_e, 2 * cap, 2 * ff), F32))

    def second_half(outs, cmat, yp, qsend, csend, lsend, yo):
        def cols(c):
            return pl.ds(pl.multiple_of(c * CC, CC), CC)

        def q_copy(c):
            return pltpu.make_async_remote_copy(
                src_ref=qsend.at[c], dst_ref=sibrecv.at[c], send_sem=qsend_sem.at[c],
                recv_sem=qrecv_sem.at[c], device_id={"ep": sib}, device_id_type=MESH)

        def c_copy(c):
            return pltpu.make_async_remote_copy(
                src_ref=csend.at[c], dst_ref=crossr_ref.at[:, cols(c)], send_sem=csend_sem.at[c],
                recv_sem=crecv_sem.at[c], device_id={"ep": far}, device_id_type=MESH)

        def l_copy(c):
            return pltpu.make_async_remote_copy(
                src_ref=lsend.at[c], dst_ref=sibr_ref.at[:, cols(c)], send_sem=lsend_sem.at[c],
                recv_sem=lrecv_sem.at[c], device_id={"ep": sib}, device_id_type=MESH)

        def o_copy(c):
            return pltpu.make_async_copy(yo.at[c], own_ref.at[:, cols(c)], osem.at[c])

        def cross_sum(c):
            q_copy(c).wait_recv()
            csend[c] = (yp[...] + sibrecv[c].astype(F32)).astype(BF16)
            c_copy(c).start()

        def combined(s, t):
            return lax.dot_general(cmat[s, :, t : t + 256], outs[s], (((0,), (0,)), ((), ())),
                                   preferred_element_type=F32)

        def down(side, h):
            def chunk(c, _):
                def body(i, _):
                    if side == 0:
                        @pl.when(i == 3)
                        def _():
                            pl.when(c > 0)(lambda: cross_sum(c - 1))
                    for b in (0, 1):
                        e = 2 * i + b
                        at = pl.ds(pl.multiple_of(e * cap, 16), cap)

                        @pl.when(c == 0)
                        def _():
                            for s in (0, 1):
                                src = 2 * (1 - side) + s
                                cmat[s, at, :] = jnp.where(
                                    slot_rows == slots_of(src, e), gates_of(src, e), 0.0).astype(BF16)
                    for b in (0, 1):
                        e = 2 * i + b
                        at = pl.ds(pl.multiple_of(e * cap, 16), cap)
                        pos = (side * nc + c) * n_e + e
                        slot = pos % DRING
                        dfilled(slot)
                        o = dot(h[e], wdr[slot]).astype(BF16)
                        outs[0, at, :] = o[:cap]
                        outs[1, at, :] = o[cap:]
                        if side == 0:
                            dfill(pos + DRING)
                        else:
                            pl.when(pos < 2 * nc * n_e - DRING)(lambda pos=pos: dfill(pos + DRING))
                    return 0

                lax.fori_loop(0, n_e // 2, body, 0)
                for s in (1, 0):
                    for t in range(0, tokens, 256):
                        y = combined(s, t)
                        if s == 1:
                            (lsend if side else qsend)[c, t : t + 256, :] = y.astype(BF16)
                        elif side:
                            yo[c, t : t + 256, :] = y
                        else:
                            yp[t : t + 256, :] = y
                if side:
                    l_copy(c).start()
                    o_copy(c).start()
                else:
                    q_copy(c).start()
                return 0

            lax.fori_loop(0, nc, chunk, 0)

        down(0, hr)

        def last_sum(i):
            pl.when(i == 0)(lambda: cross_sum(nc - 1))

        near(len(phases) - 1, late, last_sum)
        down(1, hl)
        for c in range(nc):
            q_copy(c).wait_send()
            l_copy(c).wait_send()
            l_copy(c).wait_recv()
            o_copy(c).wait()
        for c in range(nc):
            c_copy(c).wait_send()
            c_copy(c).wait_recv()

    pl.run_scoped(
        second_half,
        pltpu.VMEM((2, n_e * cap, CC), BF16),
        pltpu.VMEM((2, n_e * cap, tokens), BF16),
        pltpu.VMEM((tokens, CC), F32),
        pltpu.VMEM((nc, tokens, CC), BF16),
        pltpu.VMEM((nc, tokens, CC), BF16),
        pltpu.VMEM((nc, tokens, CC), BF16),
        pltpu.VMEM((nc, tokens, CC), F32),
    )
    for src in (1, 2, 3):
        meta_copy(src).wait_send()
        for k in range(nk):
            x_copy(src, k).wait_send()


def moe(meta, x, w_gate, w_up, w_down, cap):
    tokens, d = x.shape
    n_e, _, ff = w_gate.shape
    nk, nc = d // KC, d // CC
    dma = pltpu.SemaphoreType.DMA
    hbm = pl.BlockSpec(memory_space=pl.ANY)
    return pl.pallas_call(
        functools.partial(moe_kernel, cap),
        out_shape=[
            jax.ShapeDtypeStruct((tokens, d), F32),
            jax.ShapeDtypeStruct((tokens, d), BF16),
            jax.ShapeDtypeStruct((tokens, d), BF16),
        ],
        in_specs=[pl.BlockSpec(memory_space=pltpu.VMEM)] + [hbm] * 4,
        out_specs=[hbm] * 3,
        scratch_shapes=[
            pltpu.VMEM((4, *meta.shape), F32),
            pltpu.VMEM((4, nk, tokens, KC), BF16),
            pltpu.VMEM((RING, KC, ff), BF16),
            pltpu.VMEM((RING, KC, ff), BF16),
            pltpu.VMEM((DRING, ff, CC), BF16),
            pltpu.VMEM((n_e, 2 * cap, ff), BF16),
            pltpu.VMEM((n_e, 2 * cap, ff), BF16),
            pltpu.VMEM((nc, tokens, CC), BF16),
            pltpu.VMEM((2, 2 * cap, KC), BF16),
            pltpu.VMEM((2 * cap, d), BF16),
            dma((RING,)), dma((RING,)), dma((DRING,)), dma((nk,)),
            dma((3,)), dma((3,)), dma((3, nk)), dma((3, nk)),
            dma((nc,)), dma((nc,)), dma((nc,)), dma((nc,)), dma((nc,)), dma((nc,)), dma((nc,)),
        ],
        compiler_params=pltpu.CompilerParams(
            collective_id=0, has_side_effects=True, vmem_limit_bytes=67_043_328),
        cost_estimate=pl.CostEstimate(
            flops=24 * n_e * cap * d * ff, bytes_accessed=12 * n_e * d * ff, transcendentals=0),
    )(meta, x, w_gate, w_up, w_down)


def solution(mesh):
    members = mesh.shape["ep"]

    def local(x, expert, slot, gate, w_gate, w_up, w_down):
        x = x[0, 0]
        tokens, _ = x.shape
        top = expert.shape[-1]
        cap = 5 * tokens * top // (4 * w_gate.shape[0] * members)
        meta = jnp.concatenate(
            [expert[0, 0].T.astype(F32), jnp.minimum(slot[0, 0], cap).T.astype(F32),
             gate[0, 0].T.astype(BF16).astype(F32)], axis=0)
        own, near, far = moe(meta, x, w_gate, w_up, w_down, cap)
        y = own + near.astype(F32) + far.astype(F32)
        return y.astype(BF16)[None, None]

    tok = P("dp", "ep", None, None)
    w = P("ep", None, None)
    return jax.shard_map(local, mesh=mesh, in_specs=(tok,) * 4 + (w,) * 3, out_specs=tok, check_vma=False)
```

```python
import functools

import jax
import jax.numpy as jnp
from jax import lax
from jax.experimental import pallas as pl
from jax.experimental.pallas import tpu as pltpu
from jax.sharding import PartitionSpec as P

F32, BF16 = jnp.float32, jnp.bfloat16
MESH = pl.DeviceIdType.MESH

EARLY = 7
RING, DRING = 8, 6
KC, CC, FB = 512, 512, 256


def moe_kernel(cap, meta_ref, x_ref, wg_ref, wu_ref, wd_ref, own_ref, sibr_ref, crossr_ref,
               metas, xs, wgr, wur, wdr, hl, hr, sibrecv, zr, zl,
               gsem, usem, dsem, xsem, msend, mrecv, xsend, xrecv,
               qsend_sem, qrecv_sem, csend_sem, crecv_sem, lsend_sem, lrecv_sem, osem):
    me = lax.axis_index("ep")
    sib = me + 1 - 2 * (me % 2)
    far = (me + 2) % 4
    peers = (sib, far, (sib + 2) % 4)
    n_e, d, ff = wg_ref.shape
    top, tokens = metas.shape[1] // 3, metas.shape[2]
    nk, nc = d // KC, d // CC
    first = me * n_e

    barrier = pltpu.get_barrier_semaphore()
    for p in peers:
        pl.semaphore_signal(barrier, inc=1, device_id={"ep": p}, device_id_type=MESH)

    late = n_e - EARLY
    phases = [("L", 0, 4 * EARLY)] + [("R", k, n_e) for k in range(nk)] + [("L", EARLY, 4 * late)]
    bases = [sum(p[2] for p in phases[:i]) for i in range(len(phases))]
    total = bases[-1] + phases[-1][2]

    def piece(pos, lo):
        def inside(i):
            kind, a, _ = phases[i]
            at = pos - bases[i]
            return (a + at // 4, at % 4) if kind == "L" else (at, a)
        e, k = inside(lo)
        if lo + 1 < len(phases):
            nxt = pos // bases[lo + 1]
            e1, k1 = inside(lo + 1)
            e, k = e + nxt * (e1 - e), k + nxt * (k1 - k)
        return e, k

    def fill(pos, e, k):
        slot = pos % RING
        rows = pl.ds(pl.multiple_of(k * KC, KC), KC)
        pltpu.make_async_copy(wg_ref.at[e, rows], wgr.at[slot], gsem.at[slot]).start()
        pltpu.make_async_copy(wu_ref.at[e, rows], wur.at[slot], usem.at[slot]).start()

    def filled(slot):
        pltpu.make_async_copy(wg_ref.at[0, pl.ds(0, KC)], wgr.at[slot], gsem.at[slot]).wait()
        pltpu.make_async_copy(wu_ref.at[0, pl.ds(0, KC)], wur.at[slot], usem.at[slot]).wait()

    def dfill(pos):
        slot, e, c = pos % DRING, pos % n_e, (pos // n_e) % nc
        cols = pl.ds(pl.multiple_of(c * CC, CC), CC)
        pltpu.make_async_copy(wd_ref.at[e, :, cols], wdr.at[slot], dsem.at[slot]).start()

    def dfilled(slot):
        pltpu.make_async_copy(wd_ref.at[0, :, pl.ds(0, CC)], wdr.at[slot], dsem.at[slot]).wait()

    def x_local(k):
        return pltpu.make_async_copy(x_ref.at[:, pl.ds(k * KC, KC)], xs.at[0, k], xsem.at[k])

    def x_copy(src, k):
        piece_ref = xs.at[2 if src == 3 else 0, k]
        return pltpu.make_async_remote_copy(
            src_ref=piece_ref, dst_ref=xs.at[src, k], send_sem=xsend.at[src - 1, k],
            recv_sem=xrecv.at[src - 1, k], device_id={"ep": far if src == 2 else sib}, device_id_type=MESH)

    def meta_copy(src):
        return pltpu.make_async_remote_copy(
            src_ref=meta_ref, dst_ref=metas.at[src], send_sem=msend.at[src - 1],
            recv_sem=mrecv.at[src - 1], device_id={"ep": peers[src - 1]}, device_id_type=MESH)

    for k in range(nk):
        x_local(k).start()
    for pos in range(4):
        fill(pos, 0, pos)
    metas[0] = meta_ref[...]
    pl.semaphore_wait(barrier, 3)
    for src in (1, 2, 3):
        meta_copy(src).start()
    for k in range(nk):
        x_local(k).wait()
        if k == 0:
            x_copy(2, k).start()
        x_copy(1, k).start()
    for pos in range(4, RING):
        fill(pos, 1, pos - 4)

    slot_rows = lax.broadcasted_iota(jnp.int32, (cap, tokens), 0).astype(F32)

    def slots_of(src, e):
        hit = metas[src, 0:top, :] == (e + first).astype(F32)
        return jnp.max(jnp.where(hit, metas[src, top : 2 * top, :], -1.0), axis=0, keepdims=True)

    def gates_of(src, e):
        hit = metas[src, 0:top, :] == (e + first).astype(F32)
        return jnp.sum(jnp.where(hit, metas[src, 2 * top :, :], 0.0), axis=0, keepdims=True)

    def pick(src, e):
        return jnp.where(slot_rows == slots_of(src, e), 1.0, 0.0).astype(BF16)

    def dot(a, b):
        return jnp.dot(a, b, preferred_element_type=F32)

    def near(lo, count, after):
        _, e0, _ = phases[lo]

        def body(i, _):
            e = e0 + i
            for s in (0, 1):
                p = pick(s, e)
                for k in range(nk):
                    zl[s * cap : (s + 1) * cap, k * KC : (k + 1) * KC] = dot(p, xs[s, k]).astype(BF16)
            pos = bases[lo] + 4 * i
            at = pl.multiple_of(pos % RING, 4)
            for q in range(4):
                filled(at + q)
            for f in range(0, ff, FB):
                wg = wgr[pl.ds(at, 4), :, f : f + FB].reshape(d, FB)
                wu = wur[pl.ds(at, 4), :, f : f + FB].reshape(d, FB)
                g, u = dot(zl[...], wg), dot(zl[...], wu)
                hl[e, :, f : f + FB] = (g * jax.nn.sigmoid(g) * u).astype(BF16)

            def refill():
                for q in range(4):
                    nxt = pos + q + RING
                    fill(nxt, *piece(nxt, lo))

            if lo + 1 < len(phases):
                refill()
            else:
                pl.when(i < count - 2)(refill)
            after(i)
            return 0

        lax.fori_loop(0, count, body, 0)

    def send_next(k):
        x_copy(2, k - 1).wait_send()
        x_copy(2, k).start()

    def pass_on(k):
        x_copy(2, k).wait_recv()
        x_copy(3, k).start()

    def far_phase(k, acc):
        lo = 1 + k
        x_copy(3, k).wait_recv()

        def body(i, _):
            if k + 1 < nk:
                @pl.when(i == n_e // 2 - 1)
                def _():
                    pass_on(k + 1)
            if k + 2 < nk:
                @pl.when(i == 4 + k)
                def _():
                    send_next(k + 2)
            for b in (0, 1):
                for s in (0, 1):
                    zr[b, s * cap : (s + 1) * cap, :] = dot(pick(2 + s, 2 * i + b), xs[2 + s, k]).astype(BF16)
            for b in (0, 1):
                e = 2 * i + b
                pos = bases[lo] + e
                slot = pos % RING
                filled(slot)
                for f in range(0, ff, FB):
                    g = dot(zr[b], wgr[slot, :, f : f + FB])
                    u = dot(zr[b], wur[slot, :, f : f + FB])
                    if k:
                        g = g + acc[e, :, f : f + FB]
                        u = u + acc[e, :, ff + f : ff + f + FB]
                    if k == nk - 1:
                        hr[e, :, f : f + FB] = (g * jax.nn.sigmoid(g) * u).astype(BF16)
                    else:
                        acc[e, :, f : f + FB] = g
                        acc[e, :, ff + f : ff + f + FB] = u
                fill(pos + RING, *piece(pos + RING, lo))
            return 0

        lax.fori_loop(0, n_e // 2, body, 0)

    for k in range(nk):
        x_copy(1, k).wait_recv()
    meta_copy(1).wait_recv()

    def first_pass_on(i):
        @pl.when(i == EARLY // 2)
        def _():
            send_next(1)

        @pl.when(i == EARLY - 2)
        def _():
            pass_on(0)

    near(0, EARLY, first_pass_on)
    for pos in range(DRING):
        dfill(pos)
    meta_copy(2).wait_recv()
    meta_copy(3).wait_recv()

    def first_half(acc):
        for k in range(nk):
            far_phase(k, acc)

    pl.run_scoped(first_half, pltpu.VMEM((n_e, 2 * cap, 2 * ff), F32))

    def second_half(outs, cmat, yp, qsend, csend, lsend, yo):
        def cols(c):
            return pl.ds(pl.multiple_of(c * CC, CC), CC)

        def q_copy(c):
            return pltpu.make_async_remote_copy(
                src_ref=qsend.at[c], dst_ref=sibrecv.at[c], send_sem=qsend_sem.at[c],
                recv_sem=qrecv_sem.at[c], device_id={"ep": sib}, device_id_type=MESH)

        def c_copy(c):
            return pltpu.make_async_remote_copy(
                src_ref=csend.at[c], dst_ref=crossr_ref.at[:, cols(c)], send_sem=csend_sem.at[c],
                recv_sem=crecv_sem.at[c], device_id={"ep": far}, device_id_type=MESH)

        def l_copy(c):
            return pltpu.make_async_remote_copy(
                src_ref=lsend.at[c], dst_ref=sibr_ref.at[:, cols(c)], send_sem=lsend_sem.at[c],
                recv_sem=lrecv_sem.at[c], device_id={"ep": sib}, device_id_type=MESH)

        def o_copy(c):
            return pltpu.make_async_copy(yo.at[c], own_ref.at[:, cols(c)], osem.at[c])

        def cross_sum(c):
            q_copy(c).wait_recv()
            csend[c] = (yp[...] + sibrecv[c].astype(F32)).astype(BF16)
            c_copy(c).start()

        def combined(s, t):
            return lax.dot_general(cmat[s, :, t : t + 256], outs[s], (((0,), (0,)), ((), ())),
                                   preferred_element_type=F32)

        def down(side, h):
            def chunk(c, _):
                def body(i, _):
                    if side == 0:
                        @pl.when(i == 3)
                        def _():
                            pl.when(c > 0)(lambda: cross_sum(c - 1))
                    for b in (0, 1):
                        e = 2 * i + b
                        at = pl.ds(pl.multiple_of(e * cap, 16), cap)

                        @pl.when(c == 0)
                        def _():
                            for s in (0, 1):
                                src = 2 * (1 - side) + s
                                cmat[s, at, :] = jnp.where(
                                    slot_rows == slots_of(src, e), gates_of(src, e), 0.0).astype(BF16)
                    for b in (0, 1):
                        e = 2 * i + b
                        at = pl.ds(pl.multiple_of(e * cap, 16), cap)
                        pos = (side * nc + c) * n_e + e
                        slot = pos % DRING
                        dfilled(slot)
                        o = dot(h[e], wdr[slot]).astype(BF16)
                        outs[0, at, :] = o[:cap]
                        outs[1, at, :] = o[cap:]
                        if side == 0:
                            dfill(pos + DRING)
                        else:
                            pl.when(pos < 2 * nc * n_e - DRING)(lambda pos=pos: dfill(pos + DRING))
                    return 0

                lax.fori_loop(0, n_e // 2, body, 0)
                for s in (1, 0):
                    for t in range(0, tokens, 256):
                        y = combined(s, t)
                        if s == 1:
                            (lsend if side else qsend)[c, t : t + 256, :] = y.astype(BF16)
                        elif side:
                            yo[c, t : t + 256, :] = y
                        else:
                            yp[t : t + 256, :] = y
                if side:
                    l_copy(c).start()
                    o_copy(c).start()
                else:
                    q_copy(c).start()
                return 0

            lax.fori_loop(0, nc, chunk, 0)

        down(0, hr)

        def last_sum(i):
            pl.when(i == 0)(lambda: cross_sum(nc - 1))

        near(len(phases) - 1, late, last_sum)
        down(1, hl)
        for c in range(nc):
            q_copy(c).wait_send()
            l_copy(c).wait_send()
            l_copy(c).wait_recv()
            o_copy(c).wait()
        for c in range(nc):
            c_copy(c).wait_send()
            c_copy(c).wait_recv()

    pl.run_scoped(
        second_half,
        pltpu.VMEM((2, n_e * cap, CC), BF16),
        pltpu.VMEM((2, n_e * cap, tokens), BF16),
        pltpu.VMEM((tokens, CC), F32),
        pltpu.VMEM((nc, tokens, CC), BF16),
        pltpu.VMEM((nc, tokens, CC), BF16),
        pltpu.VMEM((nc, tokens, CC), BF16),
        pltpu.VMEM((nc, tokens, CC), F32),
    )
    for src in (1, 2, 3):
        meta_copy(src).wait_send()
        for k in range(nk):
            if src != 2 or k == nk - 1:
                x_copy(src, k).wait_send()


def moe(meta, x, w_gate, w_up, w_down, cap):
    tokens, d = x.shape
    n_e, _, ff = w_gate.shape
    nk, nc = d // KC, d // CC
    dma = pltpu.SemaphoreType.DMA
    hbm = pl.BlockSpec(memory_space=pl.ANY)
    return pl.pallas_call(
        functools.partial(moe_kernel, cap),
        out_shape=[
            jax.ShapeDtypeStruct((tokens, d), F32),
            jax.ShapeDtypeStruct((tokens, d), BF16),
            jax.ShapeDtypeStruct((tokens, d), BF16),
        ],
        in_specs=[pl.BlockSpec(memory_space=pltpu.VMEM)] + [hbm] * 4,
        out_specs=[hbm] * 3,
        scratch_shapes=[
            pltpu.VMEM((4, *meta.shape), F32),
            pltpu.VMEM((4, nk, tokens, KC), BF16),
            pltpu.VMEM((RING, KC, ff), BF16),
            pltpu.VMEM((RING, KC, ff), BF16),
            pltpu.VMEM((DRING, ff, CC), BF16),
            pltpu.VMEM((n_e, 2 * cap, ff), BF16),
            pltpu.VMEM((n_e, 2 * cap, ff), BF16),
            pltpu.VMEM((nc, tokens, CC), BF16),
            pltpu.VMEM((2, 2 * cap, KC), BF16),
            pltpu.VMEM((2 * cap, d), BF16),
            dma((RING,)), dma((RING,)), dma((DRING,)), dma((nk,)),
            dma((3,)), dma((3,)), dma((3, nk)), dma((3, nk)),
            dma((nc,)), dma((nc,)), dma((nc,)), dma((nc,)), dma((nc,)), dma((nc,)), dma((nc,)),
        ],
        compiler_params=pltpu.CompilerParams(
            collective_id=0, has_side_effects=True, vmem_limit_bytes=67_043_328),
        cost_estimate=pl.CostEstimate(
            flops=24 * n_e * cap * d * ff, bytes_accessed=12 * n_e * d * ff, transcendentals=0),
    )(meta, x, w_gate, w_up, w_down)


def solution(mesh):
    members = mesh.shape["ep"]

    def local(x, expert, slot, gate, w_gate, w_up, w_down):
        x = x[0, 0]
        tokens, _ = x.shape
        top = expert.shape[-1]
        cap = 5 * tokens * top // (4 * w_gate.shape[0] * members)
        meta = jnp.concatenate(
            [expert[0, 0].T.astype(F32), jnp.minimum(slot[0, 0], cap).T.astype(F32),
             gate[0, 0].T.astype(BF16).astype(F32)], axis=0)
        own, near, far = moe(meta, x, w_gate, w_up, w_down, cap)
        y = own + near.astype(F32) + far.astype(F32)
        return y.astype(BF16)[None, None]

    tok = P("dp", "ep", None, None)
    w = P("ep", None, None)
    return jax.shard_map(local, mesh=mesh, in_specs=(tok,) * 4 + (w,) * 3, out_specs=tok, check_vma=False)
```

```python
import functools

import jax
import jax.numpy as jnp
from jax import lax
from jax.experimental import pallas as pl
from jax.experimental.pallas import tpu as pltpu
from jax.sharding import PartitionSpec as P

F32, BF16 = jnp.float32, jnp.bfloat16
MESH = pl.DeviceIdType.MESH

RING, DRING = 4, 8
KC, CC, FB = 512, 512, 256


def moe_kernel(cap, meta_ref, x_ref, wg_ref, wu_ref, wd_ref, own_ref, sibr_ref, crossr_ref,
               metas, xs, wgr, wur, hl, zr,
               gsem, usem, dsem, xsem, msend, mrecv, xsend, xrecv,
               qsend_sem, qrecv_sem, csend_sem, crecv_sem, lsend_sem, lrecv_sem, osem, free_sem):
    me = lax.axis_index("ep")
    sib = me + 1 - 2 * (me % 2)
    far = (me + 2) % 4
    peers = (sib, far, (sib + 2) % 4)
    n_e, d, ff = wg_ref.shape
    top, tokens = metas.shape[1] // 3, metas.shape[2]
    nk, nc = d // KC, d // CC
    first = me * n_e
    near_rows, far_rows = slice(0, 2 * cap), slice(2 * cap, 4 * cap)

    barrier = pltpu.get_barrier_semaphore()
    for p in peers:
        pl.semaphore_signal(barrier, inc=1, device_id={"ep": p}, device_id_type=MESH)

    def fill(pos):
        slot, e, k = pos % RING, pos % n_e, pos // n_e
        rows = pl.ds(k * KC if isinstance(k, int) else pl.multiple_of(k * KC, KC), KC)
        pltpu.make_async_copy(wg_ref.at[e, rows], wgr.at[slot], gsem.at[slot]).start()
        pltpu.make_async_copy(wu_ref.at[e, rows], wur.at[slot], usem.at[slot]).start()

    def filled(slot):
        pltpu.make_async_copy(wg_ref.at[0, pl.ds(0, KC)], wgr.at[slot], gsem.at[slot]).wait()
        pltpu.make_async_copy(wu_ref.at[0, pl.ds(0, KC)], wur.at[slot], usem.at[slot]).wait()

    def x_local(k):
        return pltpu.make_async_copy(x_ref.at[:, pl.ds(k * KC, KC)], xs.at[k, 0], xsem.at[k])

    def x_copy(src, k):
        return pltpu.make_async_remote_copy(
            src_ref=xs.at[k, 2 if src == 3 else 0], dst_ref=xs.at[k, src], send_sem=xsend.at[src - 1, k],
            recv_sem=xrecv.at[src - 1, k], device_id={"ep": far if src == 2 else sib}, device_id_type=MESH)

    def meta_copy(src):
        return pltpu.make_async_remote_copy(
            src_ref=meta_ref, dst_ref=metas.at[src], send_sem=msend.at[src - 1],
            recv_sem=mrecv.at[src - 1], device_id={"ep": peers[src - 1]}, device_id_type=MESH)

    for k in range(nk):
        x_local(k).start()
    metas[0] = meta_ref[...]
    pl.semaphore_wait(barrier, 3)
    for src in (1, 2, 3):
        meta_copy(src).start()
    for k in range(nk):
        x_local(k).wait()
        if k == 0:
            x_copy(2, k).start()
        x_copy(1, k).start()
    for pos in range(RING):
        fill(pos)

    slot_rows = lax.broadcasted_iota(jnp.int32, (cap, tokens), 0).astype(F32)

    def slots_of(src, e):
        hit = metas[src, 0:top, :] == (e + first).astype(F32)
        return jnp.max(jnp.where(hit, metas[src, top : 2 * top, :], -1.0), axis=0, keepdims=True)

    def gates_of(src, e):
        hit = metas[src, 0:top, :] == (e + first).astype(F32)
        return jnp.sum(jnp.where(hit, metas[src, 2 * top :, :], 0.0), axis=0, keepdims=True)

    def pick(src, e):
        return jnp.where(slot_rows == slots_of(src, e), 1.0, 0.0).astype(BF16)

    def dot(a, b):
        return jnp.dot(a, b, preferred_element_type=F32)

    def far_hidden(e, half):
        block = 2 * e + half
        slab = block // 3
        return slab // 4, slab % 4, pl.ds(pl.multiple_of((block % 3) * (2 * cap), 16), 2 * cap)

    def send_next(k):
        x_copy(2, k - 1).wait_send()
        x_copy(2, k).start()

    def pass_on(k):
        x_copy(2, k).wait_recv()
        x_copy(3, k).start()

    def up_phase(k, acc):
        x_copy(1, k).wait_recv()
        x_copy(3, k).wait_recv()
        if k == nk - 1:
            for n in range(k):
                x_copy(1, n).wait_send()
                x_copy(3, n).wait_send()

        def body(i, _):
            if k + 2 < nk:
                @pl.when(i == 5)
                def _():
                    send_next(k + 2)
            if k + 1 < nk:
                @pl.when(i == n_e // 2 - 1)
                def _():
                    pass_on(k + 1)
            for src in range(4):
                both = jnp.concatenate([pick(src, 2 * i), pick(src, 2 * i + 1)], axis=0)
                z = dot(both, xs[k, src]).astype(BF16)
                zr[0, src * cap : (src + 1) * cap, :] = z[:cap]
                zr[1, src * cap : (src + 1) * cap, :] = z[cap:]
            for b in (0, 1):
                e = 2 * i + b
                pos = k * n_e + e
                slot = pos % RING
                filled(slot)
                for f in range(0, ff, FB):
                    g = dot(zr[b], wgr[slot, :, f : f + FB])
                    u = dot(zr[b], wur[slot, :, f : f + FB])
                    if k:
                        g = g + acc[e, :, f : f + FB]
                        u = u + acc[e, :, ff + f : ff + f + FB]
                    if k == nk - 1:
                        h = (g * jax.nn.sigmoid(g) * u).astype(BF16)
                        hl[e, :, f : f + FB] = h[near_rows]
                        k2, s2, rows = far_hidden(e, f // KC)
                        xs[k2, s2, rows, f % KC : f % KC + FB] = h[far_rows]
                    else:
                        acc[e, :, f : f + FB] = g
                        acc[e, :, ff + f : ff + f + FB] = u
                if k < nk - 1:
                    fill(pos + RING)
                else:
                    pl.when(e < n_e - RING)(lambda pos=pos: fill(pos + RING))
            return 0

        lax.fori_loop(0, n_e // 2, body, 0)

    for src in (1, 2, 3):
        meta_copy(src).wait_recv()
    send_next(1)
    pass_on(0)

    def first_half(acc):
        for k in range(nk):
            up_phase(k, acc)

    pl.run_scoped(first_half, pltpu.VMEM((n_e, 4 * cap, 2 * ff), F32))

    for src in (1, 2, 3):
        meta_copy(src).wait_send()
        x_copy(src, nk - 1).wait_send()
    pl.semaphore_signal(free_sem, inc=1, device_id={"ep": sib}, device_id_type=MESH)

    def second_half(wdr, outs, cmat, yp, qsend, csend, lsend, yo):
        def cols(c):
            return pl.ds(c * CC if isinstance(c, int) else pl.multiple_of(c * CC, CC), CC)

        def dfill(pos):
            slot, e, c = pos % DRING, pos % n_e, pos // n_e
            pltpu.make_async_copy(wd_ref.at[e, :, cols(c)], wdr.at[slot], dsem.at[slot]).start()

        def dfilled(slot):
            pltpu.make_async_copy(wd_ref.at[0, :, pl.ds(0, CC)], wdr.at[slot], dsem.at[slot]).wait()

        def q_copy(c):
            return pltpu.make_async_remote_copy(
                src_ref=qsend.at[c], dst_ref=xs.at[nk - 1, c], send_sem=qsend_sem.at[c],
                recv_sem=qrecv_sem.at[c], device_id={"ep": sib}, device_id_type=MESH)

        def c_copy(c):
            return pltpu.make_async_remote_copy(
                src_ref=csend.at[c], dst_ref=crossr_ref.at[:, cols(c)], send_sem=csend_sem.at[c],
                recv_sem=crecv_sem.at[c], device_id={"ep": far}, device_id_type=MESH)

        def l_copy(c):
            return pltpu.make_async_remote_copy(
                src_ref=lsend.at[c], dst_ref=sibr_ref.at[:, cols(c)], send_sem=lsend_sem.at[c],
                recv_sem=lrecv_sem.at[c], device_id={"ep": sib}, device_id_type=MESH)

        def o_copy(c):
            return pltpu.make_async_copy(yo.at[c], own_ref.at[:, cols(c)], osem.at[c])

        for pos in range(DRING):
            dfill(pos)

        def cross_sum(c):
            q_copy(c).wait_recv()
            csend[c] = (yp[...] + xs[nk - 1, c].astype(F32)).astype(BF16)
            c_copy(c).start()

        def weigh(src, e):
            at = pl.ds(pl.multiple_of(e * cap, 16), cap)
            cmat[src, at, :] = jnp.where(slot_rows == slots_of(src, e), gates_of(src, e), 0.0).astype(BF16)

        def combined(src, t):
            return lax.dot_general(cmat[src, :, t : t + 256], outs[src], (((0,), (0,)), ((), ())),
                                   preferred_element_type=F32)

        def chunk(c, _):
            def body(i, _):
                @pl.when(i == 3)
                def _():
                    pl.when(c > 0)(lambda: cross_sum(c - 1))

                @pl.when(c == 0)
                def _():
                    for b in (0, 1):
                        weigh(2, 2 * i + b)
                        weigh(3, 2 * i + b)

                for b in (0, 1):
                    e = 2 * i + b
                    at = pl.ds(pl.multiple_of(e * cap, 16), cap)
                    pos = c * n_e + e
                    slot = pos % DRING
                    dfilled(slot)
                    o = dot(hl[e], wdr[slot]).astype(BF16)
                    outs[0, at, :] = o[:cap]
                    outs[1, at, :] = o[cap:]
                    o = None
                    for half in range(ff // KC):
                        k2, s2, rows = far_hidden(e, half)
                        p = dot(xs[k2, s2, rows, :], wdr[slot, half * KC : (half + 1) * KC, :])
                        o = p if o is None else o + p
                    o = o.astype(BF16)
                    outs[2, at, :] = o[:cap]
                    outs[3, at, :] = o[cap:]
                    pl.when(pos < nc * n_e - DRING)(lambda pos=pos: dfill(pos + DRING))
                return 0

            lax.fori_loop(0, n_e // 2, body, 0)
            for t in range(0, tokens, 256):
                qsend[c, t : t + 256, :] = combined(3, t).astype(BF16)
            for t in range(0, tokens, 256):
                yp[t : t + 256, :] = combined(2, t)
            pl.when(c == 0)(lambda: pl.semaphore_wait(free_sem, 1))
            q_copy(c).start()

            @pl.when(c == 0)
            def _():
                def near_weights(e, _):
                    weigh(0, e)
                    weigh(1, e)
                    return 0

                lax.fori_loop(0, n_e, near_weights, 0)

            for t in range(0, tokens, 256):
                lsend[c, t : t + 256, :] = combined(1, t).astype(BF16)
            for t in range(0, tokens, 256):
                yo[c, t : t + 256, :] = combined(0, t)
            l_copy(c).start()
            o_copy(c).start()
            return 0

        lax.fori_loop(0, nc, chunk, 0)
        cross_sum(nc - 1)
        for c in range(nc):
            q_copy(c).wait_send()
            l_copy(c).wait_send()
            l_copy(c).wait_recv()
            o_copy(c).wait()
        for c in range(nc):
            c_copy(c).wait_send()
            c_copy(c).wait_recv()

    pl.run_scoped(
        second_half,
        pltpu.VMEM((DRING, ff, CC), BF16),
        pltpu.VMEM((4, n_e * cap, CC), BF16),
        pltpu.VMEM((4, n_e * cap, tokens), BF16),
        pltpu.VMEM((tokens, CC), F32),
        pltpu.VMEM((nc, tokens, CC), BF16),
        pltpu.VMEM((nc, tokens, CC), BF16),
        pltpu.VMEM((nc, tokens, CC), BF16),
        pltpu.VMEM((nc, tokens, CC), F32),
    )


def moe(meta, x, w_gate, w_up, w_down, cap):
    tokens, d = x.shape
    n_e, _, ff = w_gate.shape
    nk, nc = d // KC, d // CC
    dma = pltpu.SemaphoreType.DMA
    hbm = pl.BlockSpec(memory_space=pl.ANY)
    return pl.pallas_call(
        functools.partial(moe_kernel, cap),
        out_shape=[
            jax.ShapeDtypeStruct((tokens, d), F32),
            jax.ShapeDtypeStruct((tokens, d), BF16),
            jax.ShapeDtypeStruct((tokens, d), BF16),
        ],
        in_specs=[pl.BlockSpec(memory_space=pltpu.VMEM)] + [hbm] * 4,
        out_specs=[hbm] * 3,
        scratch_shapes=[
            pltpu.VMEM((4, *meta.shape), F32),
            pltpu.VMEM((nk, 4, tokens, KC), BF16),
            pltpu.VMEM((RING, KC, ff), BF16),
            pltpu.VMEM((RING, KC, ff), BF16),
            pltpu.VMEM((n_e, 2 * cap, ff), BF16),
            pltpu.VMEM((2, 4 * cap, KC), BF16),
            dma((RING,)), dma((RING,)), dma((DRING,)), dma((nk,)),
            dma((3,)), dma((3,)), dma((3, nk)), dma((3, nk)),
            dma((nc,)), dma((nc,)), dma((nc,)), dma((nc,)), dma((nc,)), dma((nc,)), dma((nc,)),
            pltpu.SemaphoreType.REGULAR,
        ],
        compiler_params=pltpu.CompilerParams(
            collective_id=0, has_side_effects=True, vmem_limit_bytes=67_043_328),
        cost_estimate=pl.CostEstimate(
            flops=24 * n_e * cap * d * ff, bytes_accessed=6 * n_e * d * ff, transcendentals=0),
    )(meta, x, w_gate, w_up, w_down)


def solution(mesh):
    members = mesh.shape["ep"]

    def local(x, expert, slot, gate, w_gate, w_up, w_down):
        x = x[0, 0]
        tokens, _ = x.shape
        top = expert.shape[-1]
        cap = 5 * tokens * top // (4 * w_gate.shape[0] * members)
        meta = jnp.concatenate(
            [expert[0, 0].T.astype(F32), jnp.minimum(slot[0, 0], cap).T.astype(F32),
             gate[0, 0].T.astype(BF16).astype(F32)], axis=0)
        own, near, far = moe(meta, x, w_gate, w_up, w_down, cap)
        y = own + near.astype(F32) + far.astype(F32)
        return y.astype(BF16)[None, None]

    tok = P("dp", "ep", None, None)
    w = P("ep", None, None)
    return jax.shard_map(local, mesh=mesh, in_specs=(tok,) * 4 + (w,) * 3, out_specs=tok, check_vma=False)
```

```python
import functools

import jax
import jax.numpy as jnp
from jax import lax
from jax.experimental import pallas as pl
from jax.experimental.pallas import tpu as pltpu
from jax.sharding import PartitionSpec as P

F32, BF16 = jnp.float32, jnp.bfloat16
MESH = pl.DeviceIdType.MESH

RING, DRING = 4, 8
KC, CC, FB = 512, 512, 256


def moe_kernel(cap, meta_ref, x_ref, wg_ref, wu_ref, wd_ref, own_ref, sibr_ref, crossr_ref,
               metas, xs, wgr, wur, hl, zr,
               gsem, usem, dsem, xsem, msend, mrecv, xsend, xrecv,
               qsend_sem, qrecv_sem, csend_sem, crecv_sem, lsend_sem, lrecv_sem, osem, free_sem):
    me = lax.axis_index("ep")
    sib = me + 1 - 2 * (me % 2)
    far = (me + 2) % 4
    peers = (sib, far, (sib + 2) % 4)
    n_e, d, ff = wg_ref.shape
    top, tokens = metas.shape[1] // 3, metas.shape[2]
    nk, nc = d // KC, d // CC
    first = me * n_e
    near_rows, far_rows = slice(0, 2 * cap), slice(2 * cap, 4 * cap)

    barrier = pltpu.get_barrier_semaphore()
    for p in peers:
        pl.semaphore_signal(barrier, inc=1, device_id={"ep": p}, device_id_type=MESH)

    def fill(pos):
        slot, e, k = pos % RING, pos % n_e, pos // n_e
        rows = pl.ds(k * KC if isinstance(k, int) else pl.multiple_of(k * KC, KC), KC)
        pltpu.make_async_copy(wg_ref.at[e, rows], wgr.at[slot], gsem.at[slot]).start()
        pltpu.make_async_copy(wu_ref.at[e, rows], wur.at[slot], usem.at[slot]).start()

    def filled(slot):
        pltpu.make_async_copy(wg_ref.at[0, pl.ds(0, KC)], wgr.at[slot], gsem.at[slot]).wait()
        pltpu.make_async_copy(wu_ref.at[0, pl.ds(0, KC)], wur.at[slot], usem.at[slot]).wait()

    def x_local(k):
        return pltpu.make_async_copy(x_ref.at[:, pl.ds(k * KC, KC)], xs.at[k, 0], xsem.at[k])

    def x_copy(src, k):
        return pltpu.make_async_remote_copy(
            src_ref=xs.at[k, 2 if src == 3 else 0], dst_ref=xs.at[k, src], send_sem=xsend.at[src - 1, k],
            recv_sem=xrecv.at[src - 1, k], device_id={"ep": far if src == 2 else sib}, device_id_type=MESH)

    def meta_copy(src):
        return pltpu.make_async_remote_copy(
            src_ref=meta_ref, dst_ref=metas.at[src], send_sem=msend.at[src - 1],
            recv_sem=mrecv.at[src - 1], device_id={"ep": peers[src - 1]}, device_id_type=MESH)

    for k in range(nk):
        x_local(k).start()
    metas[0] = meta_ref[...]
    pl.semaphore_wait(barrier, 3)
    for src in (1, 2, 3):
        meta_copy(src).start()
    for k in range(nk):
        x_local(k).wait()
        if k == 0:
            x_copy(2, k).start()
        x_copy(1, k).start()
    for pos in range(RING):
        fill(pos)

    slot_rows = lax.broadcasted_iota(jnp.int32, (cap, tokens), 0).astype(F32)

    def slots_of(src, e):
        hit = metas[src, 0:top, :] == (e + first).astype(F32)
        return jnp.max(jnp.where(hit, metas[src, top : 2 * top, :], -1.0), axis=0, keepdims=True)

    def gates_of(src, e):
        hit = metas[src, 0:top, :] == (e + first).astype(F32)
        return jnp.sum(jnp.where(hit, metas[src, 2 * top :, :], 0.0), axis=0, keepdims=True)

    def pick(src, e):
        return jnp.where(slot_rows == slots_of(src, e), 1.0, 0.0).astype(BF16)

    def dot(a, b):
        return jnp.dot(a, b, preferred_element_type=F32)

    def far_hidden(e, half):
        block = 2 * e + half
        slab = block // 3
        return slab // 4, slab % 4, pl.ds(pl.multiple_of((block % 3) * (2 * cap), 16), 2 * cap)

    def send_next(k):
        x_copy(2, k - 1).wait_send()
        x_copy(2, k).start()

    def pass_on(k):
        x_copy(2, k).wait_recv()
        x_copy(3, k).start()

    def up_phase(k, acc):
        x_copy(1, k).wait_recv()
        x_copy(3, k).wait_recv()
        if k == nk - 1:
            for n in range(k):
                x_copy(1, n).wait_send()
                x_copy(3, n).wait_send()

        def body(i, _):
            if k + 2 < nk:
                @pl.when(i == 2)
                def _():
                    send_next(k + 2)
            if k + 1 < nk:
                @pl.when(i == n_e // 4 - 1)
                def _():
                    pass_on(k + 1)
            for src in range(4):
                four = jnp.concatenate([pick(src, 4 * i + b) for b in range(4)], axis=0)
                z = dot(four, xs[k, src]).astype(BF16)
                for b in range(4):
                    zr[b, src * cap : (src + 1) * cap, :] = z[b * cap : (b + 1) * cap]
            for b in range(4):
                e = 4 * i + b
                pos = k * n_e + e
                slot = pos % RING
                filled(slot)
                for f in range(0, ff, FB):
                    g = dot(zr[b], wgr[slot, :, f : f + FB])
                    u = dot(zr[b], wur[slot, :, f : f + FB])
                    if k:
                        g = g + acc[e, :, f : f + FB]
                        u = u + acc[e, :, ff + f : ff + f + FB]
                    if k == nk - 1:
                        h = (g * jax.nn.sigmoid(g) * u).astype(BF16)
                        hl[e, :, f : f + FB] = h[near_rows]
                        k2, s2, rows = far_hidden(e, f // KC)
                        xs[k2, s2, rows, f % KC : f % KC + FB] = h[far_rows]
                    else:
                        acc[e, :, f : f + FB] = g
                        acc[e, :, ff + f : ff + f + FB] = u
                if k < nk - 1:
                    fill(pos + RING)
                else:
                    pl.when(e < n_e - RING)(lambda pos=pos: fill(pos + RING))
            return 0

        lax.fori_loop(0, n_e // 4, body, 0)

    for src in (1, 2, 3):
        meta_copy(src).wait_recv()
    send_next(1)
    pass_on(0)

    def first_half(acc):
        for k in range(nk):
            up_phase(k, acc)

    pl.run_scoped(first_half, pltpu.VMEM((n_e, 4 * cap, 2 * ff), F32))

    for src in (1, 2, 3):
        meta_copy(src).wait_send()
        x_copy(src, nk - 1).wait_send()
    pl.semaphore_signal(free_sem, inc=1, device_id={"ep": sib}, device_id_type=MESH)

    def second_half(wdr, outs, cmat, yp, qsend, csend, lsend, yo):
        def cols(c):
            return pl.ds(c * CC if isinstance(c, int) else pl.multiple_of(c * CC, CC), CC)

        def dfill(pos):
            slot, e, c = pos % DRING, pos % n_e, pos // n_e
            pltpu.make_async_copy(wd_ref.at[e, :, cols(c)], wdr.at[slot], dsem.at[slot]).start()

        def dfilled(slot):
            pltpu.make_async_copy(wd_ref.at[0, :, pl.ds(0, CC)], wdr.at[slot], dsem.at[slot]).wait()

        def q_copy(c):
            return pltpu.make_async_remote_copy(
                src_ref=qsend.at[c], dst_ref=xs.at[nk - 1, c], send_sem=qsend_sem.at[c],
                recv_sem=qrecv_sem.at[c], device_id={"ep": sib}, device_id_type=MESH)

        def c_copy(c):
            return pltpu.make_async_remote_copy(
                src_ref=csend.at[c], dst_ref=crossr_ref.at[c], send_sem=csend_sem.at[c],
                recv_sem=crecv_sem.at[c], device_id={"ep": far}, device_id_type=MESH)

        def l_copy(c):
            return pltpu.make_async_remote_copy(
                src_ref=lsend.at[c], dst_ref=sibr_ref.at[c], send_sem=lsend_sem.at[c],
                recv_sem=lrecv_sem.at[c], device_id={"ep": sib}, device_id_type=MESH)

        def o_copy(c):
            return pltpu.make_async_copy(yo.at[c], own_ref.at[:, cols(c)], osem.at[c])

        for pos in range(DRING):
            dfill(pos)

        def cross_sum(c):
            q_copy(c).wait_recv()
            csend[c] = (yp[...] + xs[nk - 1, c].astype(F32)).astype(BF16)
            c_copy(c).start()

        def weigh(src, e):
            at = pl.ds(pl.multiple_of(e * cap, 16), cap)
            cmat[src, at, :] = jnp.where(slot_rows == slots_of(src, e), gates_of(src, e), 0.0).astype(BF16)

        def combined(src, t):
            return lax.dot_general(cmat[src, :, t : t + 256], outs[src], (((0,), (0,)), ((), ())),
                                   preferred_element_type=F32)

        def chunk(c, _):
            def body(i, _):
                @pl.when(i == 3)
                def _():
                    pl.when(c > 0)(lambda: cross_sum(c - 1))

                @pl.when(c == 0)
                def _():
                    for b in (0, 1):
                        weigh(2, 2 * i + b)
                        weigh(3, 2 * i + b)

                for b in (0, 1):
                    e = 2 * i + b
                    at = pl.ds(pl.multiple_of(e * cap, 16), cap)
                    pos = c * n_e + e
                    slot = pos % DRING
                    dfilled(slot)
                    o = None
                    for half in range(ff // KC):
                        k2, s2, rows = far_hidden(e, half)
                        part = slice(half * KC, (half + 1) * KC)
                        h = jnp.concatenate([hl[e, :, part], xs[k2, s2, rows, :]], axis=0)
                        p = dot(h, wdr[slot, part, :])
                        o = p if o is None else o + p
                    o = o.astype(BF16)
                    for src in range(4):
                        outs[src, at, :] = o[src * cap : (src + 1) * cap]
                    pl.when(pos < nc * n_e - DRING)(lambda pos=pos: dfill(pos + DRING))
                return 0

            lax.fori_loop(0, n_e // 2, body, 0)
            for t in range(0, tokens, 256):
                qsend[c, t : t + 256, :] = combined(3, t).astype(BF16)
            for t in range(0, tokens, 256):
                yp[t : t + 256, :] = combined(2, t)
            pl.when(c == 0)(lambda: pl.semaphore_wait(free_sem, 1))
            q_copy(c).start()

            @pl.when(c == 0)
            def _():
                def near_weights(e, _):
                    weigh(0, e)
                    weigh(1, e)
                    return 0

                lax.fori_loop(0, n_e, near_weights, 0)

            for t in range(0, tokens, 256):
                lsend[c, t : t + 256, :] = combined(1, t).astype(BF16)
            for t in range(0, tokens, 256):
                yo[c, t : t + 256, :] = combined(0, t)
            l_copy(c).start()
            o_copy(c).start()
            return 0

        lax.fori_loop(0, nc, chunk, 0)
        cross_sum(nc - 1)
        for c in range(nc):
            q_copy(c).wait_send()
            l_copy(c).wait_send()
            l_copy(c).wait_recv()
            o_copy(c).wait()
        for c in range(nc):
            c_copy(c).wait_send()
            c_copy(c).wait_recv()

    pl.run_scoped(
        second_half,
        pltpu.VMEM((DRING, ff, CC), BF16),
        pltpu.VMEM((4, n_e * cap, CC), BF16),
        pltpu.VMEM((4, n_e * cap, tokens), BF16),
        pltpu.VMEM((tokens, CC), F32),
        pltpu.VMEM((nc, tokens, CC), BF16),
        pltpu.VMEM((nc, tokens, CC), BF16),
        pltpu.VMEM((nc, tokens, CC), BF16),
        pltpu.VMEM((nc, tokens, CC), F32),
    )


def moe(meta, x, w_gate, w_up, w_down, cap):
    tokens, d = x.shape
    n_e, _, ff = w_gate.shape
    nk, nc = d // KC, d // CC
    dma = pltpu.SemaphoreType.DMA
    hbm = pl.BlockSpec(memory_space=pl.ANY)
    return pl.pallas_call(
        functools.partial(moe_kernel, cap),
        out_shape=[
            jax.ShapeDtypeStruct((tokens, d), F32),
            jax.ShapeDtypeStruct((nc, tokens, CC), BF16),
            jax.ShapeDtypeStruct((nc, tokens, CC), BF16),
        ],
        in_specs=[pl.BlockSpec(memory_space=pltpu.VMEM)] + [hbm] * 4,
        out_specs=[hbm] * 3,
        scratch_shapes=[
            pltpu.VMEM((4, *meta.shape), F32),
            pltpu.VMEM((nk, 4, tokens, KC), BF16),
            pltpu.VMEM((RING, KC, ff), BF16),
            pltpu.VMEM((RING, KC, ff), BF16),
            pltpu.VMEM((n_e, 2 * cap, ff), BF16),
            pltpu.VMEM((4, 4 * cap, KC), BF16),
            dma((RING,)), dma((RING,)), dma((DRING,)), dma((nk,)),
            dma((3,)), dma((3,)), dma((3, nk)), dma((3, nk)),
            dma((nc,)), dma((nc,)), dma((nc,)), dma((nc,)), dma((nc,)), dma((nc,)), dma((nc,)),
            pltpu.SemaphoreType.REGULAR,
        ],
        compiler_params=pltpu.CompilerParams(
            collective_id=0, has_side_effects=True, vmem_limit_bytes=67_043_328),
        cost_estimate=pl.CostEstimate(
            flops=24 * n_e * cap * d * ff, bytes_accessed=6 * n_e * d * ff, transcendentals=0),
    )(meta, x, w_gate, w_up, w_down)


def total_kernel(own_ref, near_ref, far_ref, y_ref):
    y_ref[...] = (own_ref[...] + near_ref[0].astype(F32) + far_ref[0].astype(F32)).astype(BF16)


def total(own, near, far):
    tokens, d = own.shape
    rows = tokens // 2
    flat = pl.BlockSpec((rows, CC), lambda c, r: (r, c))
    piece = pl.BlockSpec((1, rows, CC), lambda c, r: (c, r, 0))
    return pl.pallas_call(
        total_kernel,
        grid=(d // CC, 2),
        out_shape=jax.ShapeDtypeStruct((tokens, d), BF16),
        in_specs=[flat, piece, piece],
        out_specs=flat,
        cost_estimate=pl.CostEstimate(flops=2 * tokens * d, bytes_accessed=10 * tokens * d, transcendentals=0),
    )(own, near, far)


def solution(mesh):
    members = mesh.shape["ep"]

    def local(x, expert, slot, gate, w_gate, w_up, w_down):
        x = x[0, 0]
        tokens, _ = x.shape
        top = expert.shape[-1]
        cap = 5 * tokens * top // (4 * w_gate.shape[0] * members)
        meta = jnp.concatenate(
            [expert[0, 0].T.astype(F32), jnp.minimum(slot[0, 0], cap).T.astype(F32),
             gate[0, 0].T.astype(BF16).astype(F32)], axis=0)
        own, near, far = moe(meta, x, w_gate, w_up, w_down, cap)
        y = total(own, near, far)
        return y[None, None]

    tok = P("dp", "ep", None, None)
    w = P("ep", None, None)
    return jax.shard_map(local, mesh=mesh, in_specs=(tok,) * 4 + (w,) * 3, out_specs=tok, check_vma=False)
```
